1024 devices in a mesh: row: 16 (over y, core), col: 64 (over x, z).
Axes of the slice: x: 4, y: 8, z: 16, core: 2. Of those that a mesh axis runs over, the one named last changes fastest.
Arguments:
- matrix: float32 [16384, 16384], P('row', 'col'), may hold values from -1 to 4, as said below
Outputs:
- reduced: float32 [16384, 16384], P('row', 'col')
The draws below stay inside these ranges and needn't reach their ends.
Inputs may be any that keep to these rules, and one draw needn't show every extreme that they name: matrix is symmetric; its diagonal entries lie between 1 and 3 up to entries of size about 16384^-1/2 that every entry carries; entries at distance 256 from the diagonal with the smaller index under 2 * 256 carry an added 2.
All inputs are finite; a program needn't handle non-finite values.
Results may differ from the reference program's by a relative error of at most 0.00019.
Values sent between devices are 32-bit elements; how exact they have to be, the bound alone decides.
No kernel may reach another device: no remote copies, remote signals or barrier semaphores. Data moves between devices by JAX's collectives and lax.ppermute only.
A program may use at most 32 MiB of HBM per device.

```python
import math
import jax
import jax.numpy as jnp
from jax import lax

B = 256
PANELS = 1
N = 16384


def draw_matrix(key, part):
    first_key = jax.random.fold_in(key, 11)
    second_key = jax.random.fold_in(key, 23)
    noise = jax.random.normal(first_key, (N, N), jnp.float32)
    noise = (noise + noise.T) * (0.7071 / math.sqrt(N))
    diagonal = jax.random.uniform(second_key, (N,), jnp.float32, 1.0, 3.0)
    all_rows = jnp.arange(N, dtype=jnp.int32)
    apart = jnp.abs(all_rows[:, None] - all_rows[None, :]) == B
    early = jnp.minimum(all_rows[:, None], all_rows[None, :]) < 2 * B
    banded = jnp.where(apart & early, 2.0, 0.0)
    return noise + jnp.diag(diagonal) + banded


def setup_inputs(seed: int = 0) -> dict:
    keys = jax.random.split(jax.random.key(seed), 2)
    return {
        "matrix": draw_matrix(jax.random.fold_in(keys[1], 71), 0),
    }


def product(left, right):
    return jnp.dot(left.astype(jnp.float32), right.astype(jnp.float32), precision=lax.Precision.HIGHEST, preferred_element_type=jnp.float32)

def left_product(left, right):
    return lax.dot_general(left.astype(jnp.float32), right.astype(jnp.float32), (((0,), (0,)), ((), ())), precision=lax.Precision.HIGHEST, preferred_element_type=jnp.float32)

def right_product(left, right):
    return lax.dot_general(left.astype(jnp.float32), right.astype(jnp.float32), (((1,), (1,)), ((), ())), precision=lax.Precision.HIGHEST, preferred_element_type=jnp.float32)

def factor_inverse(kmat):
    cholesky_low = jnp.linalg.cholesky(left_product(kmat, kmat))
    halfway = lax.linalg.triangular_solve(cholesky_low, kmat.T, left_side=True, lower=True)
    return lax.linalg.triangular_solve(cholesky_low, halfway, left_side=True, lower=True, transpose_a=True)

def reference(matrix):
    current = matrix
    all_rows = jnp.arange(N, dtype=jnp.int32)
    columns = jnp.arange(B, dtype=jnp.int32)
    identity = jnp.eye(B, dtype=jnp.float32)
    for panel_index in range(PANELS):
        start_row = (panel_index + 1) * B
        sign = 1.0 if panel_index % 2 == 0 else -1.0
        panel = current[:, panel_index * B:(panel_index + 1) * B]
        panel = jnp.where((all_rows >= start_row)[:, None], panel, 0.0)
        top = panel[start_row:start_row + B]
        gram = left_product(panel, panel)
        cholesky_low = jnp.linalg.cholesky(gram)
        ortho = lax.linalg.triangular_solve(cholesky_low, panel, left_side=False, lower=True, transpose_a=True)
        top_q = lax.linalg.triangular_solve(cholesky_low, top, left_side=False, lower=True, transpose_a=True)
        tfac = factor_inverse(identity + sign * top_q)
        unit = (all_rows[:, None] - start_row == columns[None, :]).astype(jnp.float32)
        refl = ortho + sign * unit
        x_all = product(current, refl)
        y_full = left_product(refl, x_all)
        middle = product(product(tfac.T, y_full), tfac)
        w_all = product(x_all, tfac) - 0.5 * product(refl, middle)
        current = current - right_product(w_all, refl) - right_product(refl, w_all)
    return current
```

```python
import jax
import jax.numpy as jnp
from jax import lax
from jax.experimental import pallas as pl
from jax.experimental.pallas import tpu as pltpu
from jax.sharding import Mesh
from jax.sharding import PartitionSpec as P

ROW = ("y", "core")
COL = ("x", "z")
EVERY = ROW + COL
SIGN = 1.0


def dot(left, right, dims):
    return lax.dot_general(
        left,
        right,
        (dims, ((), ())),
        precision=lax.Precision.HIGHEST,
        preferred_element_type=jnp.float32,
    )


def mm(left, right):
    return dot(left, right, ((1,), (0,)))


def tn(left, right):
    return dot(left, right, ((0,), (0,)))


def nt(left, right):
    return dot(left, right, ((1,), (1,)))


def exchange(tiles, axis):
    return lax.all_to_all(tiles, axis, 0, 0, tiled=True)


def to_all(piece, axis):
    n = lax.axis_size(axis)
    return exchange(jnp.broadcast_to(piece[None], (n, *piece.shape)), axis)


def invert_half(m_ref, c_ref):
    n = m_ref.shape[0]
    lanes = lax.broadcasted_iota(jnp.int32, (n, n), 1)
    subs = lax.broadcasted_iota(jnp.int32, (n, n), 0)
    lane_row = lax.broadcasted_iota(jnp.int32, (1, n), 1)

    def step(k, carry):
        m = m_ref[...]
        hit = lanes == k
        col = jnp.sum(jnp.where(hit, m, 0.0), axis=1, keepdims=True)
        c_ref[...] = jnp.broadcast_to(col, (n, n))
        pivot = c_ref[pl.ds(k, 1), :]
        row = jnp.where(lane_row == k, 1.0, m_ref[pl.ds(k, 1), :]) / pivot
        rest = jnp.where(hit, 0.0, m) - c_ref[...] * row
        m_ref[...] = jnp.where(subs == k, row, rest)
        return carry

    lax.fori_loop(0, n, step, 0)


def inverse_kernel(a_ref, out_ref, m_ref, c_ref):
    h = a_ref.shape[0] // 2
    a12 = a_ref[:h, h:]
    a21 = a_ref[h:, :h]
    m_ref[...] = a_ref[:h, :h]
    invert_half(m_ref, c_ref)
    t11 = m_ref[...]
    right = mm(t11, a12)
    left = mm(a21, t11)
    m_ref[...] = a_ref[h:, h:] - mm(a21, right)
    invert_half(m_ref, c_ref)
    t22 = m_ref[...]
    up = mm(right, t22)
    out_ref[:h, :h] = t11 + mm(up, left)
    out_ref[:h, h:] = -up
    out_ref[h:, :h] = -mm(t22, left)
    out_ref[h:, h:] = t22


def inverse(a):
    n = a.shape[0]
    return pl.pallas_call(
        inverse_kernel,
        out_shape=jax.ShapeDtypeStruct(a.shape, jnp.float32),
        scratch_shapes=[
            pltpu.VMEM((n // 2, n // 2), jnp.float32),
            pltpu.VMEM((n // 2, n // 2), jnp.float32),
        ],
        cost_estimate=pl.CostEstimate(
            flops=100_000_000, bytes_accessed=3 * a.size * 4, transcendentals=0
        ),
    )(a)


def per_device(matrix):
    row_count, width = matrix.shape
    rows, xs, zs = lax.axis_size(ROW), lax.axis_size("x"), lax.axis_size("z")
    part = width // rows
    ratio = row_count // width
    row_id = lax.axis_index(ROW)
    col_id = lax.axis_index(COL)
    cols = xs * zs

    def to_block_row(piece):
        pairs = []
        for r in range(rows):
            for c in range(cols):
                pairs.append((r * cols + c, (c // ratio) * cols + (c % ratio) * rows + r))
        return lax.ppermute(piece, EVERY, pairs)

    first = (row_id == 0).astype(jnp.float32)

    panel_c0 = jnp.where(col_id > 0, matrix[:width].T, 0.0)
    piece = exchange(panel_c0.reshape(rows, part, width), ROW)[0]
    along_z = to_all(to_block_row(piece), "z").reshape(zs * part, width)
    panel_r = to_all(along_z, "x").reshape(row_count, width)

    gram_r = tn(panel_r, panel_r)
    top_r = panel_r[width : 2 * width] * first
    both = jnp.concatenate(
        [gram_r.reshape(rows, part, width), top_r.reshape(rows, part, width)], axis=1
    )
    both = jnp.sum(exchange(both, ROW), axis=0)
    three = to_all(jnp.concatenate([both, piece], axis=0), ROW)
    gram = three[:, :part].reshape(width, width)
    top = three[:, part : 2 * part].reshape(width, width)
    panel_c = three[:, 2 * part :].reshape(width, width)

    low = jnp.linalg.cholesky(gram)
    upper = SIGN * low.T
    refl_c = panel_c + jnp.where(col_id == 1, upper, 0.0)
    refl_r = lax.dynamic_update_slice_in_dim(
        panel_r, panel_r[width : 2 * width] + first * upper, width, 0
    )

    x_part = tn(matrix, refl_r)
    y_part = tn(refl_c, x_part)
    both = jnp.concatenate(
        [x_part.reshape(rows, part, width), y_part.reshape(rows, part, width)], axis=1
    )
    both = jnp.sum(exchange(both, ROW), axis=0)
    x_piece, y_piece = both[:part], both[part:]
    x_moved = to_block_row(x_piece)
    tfac = inverse(gram + SIGN * mm(low, top))
    both = to_all(jnp.concatenate([x_moved, y_piece], axis=0), "z")
    x_z = both[:, :part].reshape(zs * part, width)
    y_z = jnp.sum(both[:, part:], axis=0)
    both = to_all(jnp.concatenate([x_z, y_z], axis=0), "x")
    x_r = both[:, : zs * part].reshape(row_count, width)
    y_piece = jnp.sum(both[:, zs * part :], axis=0)
    both = to_all(jnp.concatenate([x_piece, y_piece], axis=0), ROW)
    x_c = both[:, :part].reshape(width, width)
    y_full = both[:, part:].reshape(width, width)

    middle = tn(tfac, mm(y_full, tfac))
    side = mm(x_c, tfac) - mm(refl_c, middle)
    lead = nt(refl_c, tfac)
    return matrix - nt(x_r, lead) - nt(refl_r, side)


def solution(mesh):
    shape = (mesh.shape["row"] // 2, 2, 4, mesh.shape["col"] // 4)
    torus = Mesh(mesh.devices.reshape(shape), EVERY)
    return jax.shard_map(
        per_device,
        mesh=torus,
        in_specs=(P(ROW, COL),),
        out_specs=P(ROW, COL),
        check_vma=False,
    )
```

```python
import jax
import jax.numpy as jnp
from jax import lax
from jax.experimental import pallas as pl
from jax.experimental.pallas import tpu as pltpu
from jax.sharding import Mesh
from jax.sharding import PartitionSpec as P

ROW = ("y", "core")
COL = ("x", "z")
EVERY = ROW + COL
SIGN = 1.0


def dot(left, right, dims, precision):
    return lax.dot_general(
        left,
        right,
        (dims, ((), ())),
        precision=precision,
        preferred_element_type=jnp.float32,
    )


def mm(left, right, precision=lax.Precision.HIGHEST):
    return dot(left, right, ((1,), (0,)), precision)


def tn(left, right, precision=lax.Precision.HIGHEST):
    return dot(left, right, ((0,), (0,)), precision)


def nt(left, right, precision=lax.Precision.HIGHEST):
    return dot(left, right, ((1,), (1,)), precision)


def exchange(tiles, axis):
    return lax.all_to_all(tiles, axis, 0, 0, tiled=True)


def to_all(piece, axis):
    n = lax.axis_size(axis)
    return exchange(jnp.broadcast_to(piece[None], (n, *piece.shape)), axis)


def invert_half(m_ref, c_ref):
    n = m_ref.shape[0]
    lanes = lax.broadcasted_iota(jnp.int32, (n, n), 1)
    subs = lax.broadcasted_iota(jnp.int32, (n, n), 0)
    lane_row = lax.broadcasted_iota(jnp.int32, (1, n), 1)

    def step(k, carry):
        m = m_ref[...]
        hit = lanes == k
        col = jnp.sum(jnp.where(hit, m, 0.0), axis=1, keepdims=True)
        c_ref[...] = jnp.broadcast_to(col, (n, n))
        pivot = c_ref[pl.ds(k, 1), :]
        row = jnp.where(lane_row == k, 1.0, m_ref[pl.ds(k, 1), :]) / pivot
        rest = jnp.where(hit, 0.0, m) - c_ref[...] * row
        m_ref[...] = jnp.where(subs == k, row, rest)
        return carry

    lax.fori_loop(0, n, step, 0)


def first_half(a_ref, t11_ref, right_ref, left_ref, schur_ref, m_ref, c_ref):
    h = a_ref.shape[0] // 2
    m_ref[...] = a_ref[:h, :h]
    invert_half(m_ref, c_ref)
    t11 = m_ref[...]
    right = mm(t11, a_ref[:h, h:])
    t11_ref[...] = t11
    right_ref[...] = right
    left_ref[...] = mm(a_ref[h:, :h], t11)
    schur_ref[...] = a_ref[h:, h:] - mm(a_ref[h:, :h], right)


def second_half(t11_ref, right_ref, left_ref, schur_ref, out_ref, m_ref, c_ref):
    h = t11_ref.shape[0]
    m_ref[...] = schur_ref[...]
    invert_half(m_ref, c_ref)
    t22 = m_ref[...]
    up = mm(right_ref[...], t22)
    out_ref[:h, :h] = t11_ref[...] + mm(up, left_ref[...])
    out_ref[:h, h:] = -up
    out_ref[h:, :h] = -mm(t22, left_ref[...])
    out_ref[h:, h:] = t22


COST = pl.CostEstimate(flops=2_000_000_000, bytes_accessed=500_000, transcendentals=0)


def half_inverted(a):
    half = jax.ShapeDtypeStruct((a.shape[0] // 2, a.shape[1] // 2), jnp.float32)
    return pl.pallas_call(
        first_half,
        out_shape=[half] * 4,
        scratch_shapes=[pltpu.VMEM(half.shape, jnp.float32)] * 2,
        cost_estimate=COST,
    )(a)


def inverted(parts):
    h = parts[0].shape[0]
    return pl.pallas_call(
        second_half,
        out_shape=jax.ShapeDtypeStruct((2 * h, 2 * h), jnp.float32),
        scratch_shapes=[pltpu.VMEM((h, h), jnp.float32)] * 2,
        cost_estimate=COST,
    )(*parts)


def per_device(matrix):
    row_count, width = matrix.shape
    rows, xs, zs = lax.axis_size(ROW), lax.axis_size("x"), lax.axis_size("z")
    part = width // rows
    ratio = row_count // width
    row_id = lax.axis_index(ROW)
    col_id = lax.axis_index(COL)
    cols = xs * zs

    def to_block_row(piece):
        pairs = []
        for r in range(rows):
            for c in range(cols):
                pairs.append((r * cols + c, (c // ratio) * cols + (c % ratio) * rows + r))
        return lax.ppermute(piece, EVERY, pairs)

    first = (row_id == 0).astype(jnp.float32)
    fast = lax.Precision.HIGH

    panel_c0 = jnp.where(col_id > 0, matrix[:width].T, 0.0)
    head, below = matrix[:width], matrix[width:]
    gram_r = tn(below, below) + tn(head * (1.0 - first), head)
    both = exchange(
        jnp.concatenate(
            [panel_c0.reshape(rows, part, width), gram_r.reshape(rows, part, width)], axis=1
        ),
        ROW,
    )
    piece = both[0, :part]
    gram_piece = jnp.sum(both[:, part:], axis=0)
    moved = to_block_row(piece)

    lead = to_all(jnp.where(col_id == 0, gram_piece, piece), "x")[0]
    lead = to_all(lead, "z")[:2].reshape(2 * part, width)
    lead = to_all(jnp.concatenate([lead, piece], axis=0), ROW)
    lead, moved = lax.optimization_barrier((lead, moved))
    gram = lead[:, :part].reshape(width, width)
    top = lead[:, part : 2 * part].reshape(width, width)
    panel_c = lead[:, 2 * part :].reshape(width, width)

    along_z = to_all(moved, "z").reshape(zs * part, width)
    panel_r = to_all(along_z, "x").reshape(row_count, width)
    low = lax.linalg.cholesky(gram, symmetrize_input=False)
    upper = SIGN * low.T
    parts = half_inverted(gram + SIGN * mm(low, top))
    refl_c = panel_c + jnp.where(col_id == 1, upper, 0.0)
    refl_r = lax.dynamic_update_slice_in_dim(
        panel_r, panel_r[width : 2 * width] + first * upper, width, 0
    )

    x_part = tn(matrix, refl_r, fast)
    y_part = tn(refl_c, x_part)
    both = jnp.concatenate(
        [x_part.reshape(rows, part, width), y_part.reshape(rows, part, width)], axis=1
    )
    both = jnp.sum(exchange(both, ROW), axis=0)
    x_piece, y_piece = both[:part], both[part:]
    x_moved = to_block_row(x_piece)
    y_z = to_all(y_piece, "z")
    x_moved, y_z = lax.optimization_barrier((x_moved, y_z))
    y_z = jnp.sum(y_z, axis=0)
    x_z = to_all(x_moved, "z").reshape(zs * part, width)
    both, parts = lax.optimization_barrier((jnp.concatenate([x_z, y_z], axis=0), parts))
    both = to_all(both, "x")
    tfac = inverted(parts)
    x_r = both[:, : zs * part].reshape(row_count, width)
    y_piece = jnp.sum(both[:, zs * part :], axis=0)
    both = jnp.concatenate([x_piece, y_piece], axis=0)
    both, tfac = lax.optimization_barrier((both, tfac))
    both = to_all(both, ROW)
    x_c = both[:, :part].reshape(width, width)
    y_full = both[:, part:].reshape(width, width)

    middle = tn(tfac, mm(y_full, tfac))
    side = mm(x_c, tfac) - mm(refl_c, middle)
    lead = nt(refl_c, tfac)
    return matrix - nt(x_r, lead, fast) - nt(refl_r, side, fast)


def solution(mesh):
    shape = (mesh.shape["row"] // 2, 2, 4, mesh.shape["col"] // 4)
    torus = Mesh(mesh.devices.reshape(shape), EVERY)
    return jax.shard_map(
        per_device,
        mesh=torus,
        in_specs=(P(ROW, COL),),
        out_specs=P(ROW, COL),
        check_vma=False,
    )
```

```python
import jax
import jax.numpy as jnp
from jax import lax
from jax.experimental import pallas as pl
from jax.experimental.pallas import tpu as pltpu
from jax.sharding import Mesh
from jax.sharding import PartitionSpec as P

ROW = ("y", "core")
COL = ("x", "z")
EVERY = ROW + COL
SIGN = 1.0


def dot(left, right, dims, precision):
    return lax.dot_general(
        left,
        right,
        (dims, ((), ())),
        precision=precision,
        preferred_element_type=jnp.float32,
    )


def mm(left, right, precision=lax.Precision.HIGHEST):
    return dot(left, right, ((1,), (0,)), precision)


def tn(left, right, precision=lax.Precision.HIGHEST):
    return dot(left, right, ((0,), (0,)), precision)


def nt(left, right, precision=lax.Precision.HIGHEST):
    return dot(left, right, ((1,), (1,)), precision)


def exchange(tiles, axis):
    return lax.all_to_all(tiles, axis, 0, 0, tiled=True)


def to_all(piece, axis):
    n = lax.axis_size(axis)
    return exchange(jnp.broadcast_to(piece[None], (n, *piece.shape)), axis)


def invert_half(m_ref, c_ref):
    n = m_ref.shape[0]
    lanes = lax.broadcasted_iota(jnp.int32, (n, n), 1)
    subs = lax.broadcasted_iota(jnp.int32, (n, n), 0)
    lane_row = lax.broadcasted_iota(jnp.int32, (1, n), 1)

    def step(k, carry):
        m = m_ref[...]
        hit = lanes == k
        col = jnp.sum(jnp.where(hit, m, 0.0), axis=1, keepdims=True)
        c_ref[...] = jnp.broadcast_to(col, (n, n))
        pivot = c_ref[pl.ds(k, 1), :]
        row = jnp.where(lane_row == k, 1.0, m_ref[pl.ds(k, 1), :]) / pivot
        rest = jnp.where(hit, 0.0, m) - c_ref[...] * row
        m_ref[...] = jnp.where(subs == k, row, rest)
        return carry

    lax.fori_loop(0, n, step, 0)


def first_half(a_ref, t11_ref, right_ref, left_ref, schur_ref, m_ref, c_ref):
    h = a_ref.shape[0] // 2
    m_ref[...] = a_ref[:h, :h]
    invert_half(m_ref, c_ref)
    t11 = m_ref[...]
    right = mm(t11, a_ref[:h, h:])
    t11_ref[...] = t11
    right_ref[...] = right
    left_ref[...] = mm(a_ref[h:, :h], t11)
    schur_ref[...] = a_ref[h:, h:] - mm(a_ref[h:, :h], right)


def second_half(t11_ref, right_ref, left_ref, schur_ref, out_ref, m_ref, c_ref):
    h = t11_ref.shape[0]
    m_ref[...] = schur_ref[...]
    invert_half(m_ref, c_ref)
    t22 = m_ref[...]
    up = mm(right_ref[...], t22)
    out_ref[:h, :h] = t11_ref[...] + mm(up, left_ref[...])
    out_ref[:h, h:] = -up
    out_ref[h:, :h] = -mm(t22, left_ref[...])
    out_ref[h:, h:] = t22


COST = pl.CostEstimate(flops=2_000_000_000, bytes_accessed=500_000, transcendentals=0)


def half_inverted(a):
    half = jax.ShapeDtypeStruct((a.shape[0] // 2, a.shape[1] // 2), jnp.float32)
    return pl.pallas_call(
        first_half,
        out_shape=[half] * 4,
        scratch_shapes=[pltpu.VMEM(half.shape, jnp.float32)] * 2,
        cost_estimate=COST,
    )(a)


def inverted(parts):
    h = parts[0].shape[0]
    return pl.pallas_call(
        second_half,
        out_shape=jax.ShapeDtypeStruct((2 * h, 2 * h), jnp.float32),
        scratch_shapes=[pltpu.VMEM((h, h), jnp.float32)] * 2,
        cost_estimate=COST,
    )(*parts)


def per_device(matrix):
    row_count, width = matrix.shape
    rows, xs, zs = lax.axis_size(ROW), lax.axis_size("x"), lax.axis_size("z")
    part = width // rows
    ratio = row_count // width
    row_id = lax.axis_index(ROW)
    col_id = lax.axis_index(COL)
    cols = xs * zs

    def to_block_row(piece):
        pairs = []
        for r in range(rows):
            for c in range(cols):
                pairs.append((r * cols + c, (c // ratio) * cols + (c % ratio) * rows + r))
        return lax.ppermute(piece, EVERY, pairs)

    first = (row_id == 0).astype(jnp.float32)
    fast = lax.Precision.HIGH

    panel_c0 = jnp.where(col_id > 0, matrix[:width].T, 0.0)
    head, below = matrix[:width], matrix[width:]
    gram_r = tn(below, below) + tn(head * (1.0 - first), head)
    both = exchange(
        jnp.concatenate(
            [panel_c0.reshape(rows, part, width), gram_r.reshape(rows, part, width)], axis=1
        ),
        ROW,
    )
    piece = both[0, :part]
    gram_piece = jnp.sum(both[:, part:], axis=0)
    moved = to_block_row(piece)

    lead = to_all(jnp.where(col_id == 0, gram_piece, piece), "x")[0]
    lead = to_all(lead, "z")[:2].reshape(2 * part, width)
    lead = to_all(lead, ROW)
    lead, moved = lax.optimization_barrier((lead, moved))
    gram = lead[:, :part].reshape(width, width)
    top = lead[:, part:].reshape(width, width)

    along_z = to_all(moved, "z").reshape(zs * part, width)
    panel_r = to_all(along_z, "x").reshape(row_count, width)
    low = lax.linalg.cholesky(gram, symmetrize_input=False)
    upper = SIGN * low.T
    parts = half_inverted(gram + SIGN * mm(low, top))
    refl_r = lax.dynamic_update_slice_in_dim(
        panel_r, panel_r[width : 2 * width] + first * upper, width, 0
    )

    x_part = tn(matrix, refl_r, fast)
    x_piece = jnp.sum(exchange(x_part.reshape(rows, part, width), ROW), axis=0)
    x_moved = to_block_row(x_piece)
    both = to_all(jnp.concatenate([x_piece, piece], axis=0), ROW)
    x_moved, both = lax.optimization_barrier((x_moved, both))
    x_c = both[:, :part].reshape(width, width)
    refl_c = both[:, part:].reshape(width, width) + jnp.where(col_id == 1, upper, 0.0)
    x_z = to_all(x_moved, "z").reshape(zs * part, width)
    x_z, parts = lax.optimization_barrier((x_z, parts))
    x_r = to_all(x_z, "x").reshape(row_count, width)
    tfac = inverted(parts)
    x_r, tfac = lax.optimization_barrier((x_r, tfac))

    y_part = tn(refl_r, x_r, fast)
    y_piece = jnp.sum(exchange(y_part.reshape(rows, part, width), ROW), axis=0)
    y_full = to_all(y_piece, ROW).reshape(width, width)

    middle = tn(tfac, mm(y_full, tfac))
    side = mm(x_c, tfac) - mm(refl_c, middle)
    lead = nt(refl_c, tfac)
    return matrix - nt(x_r, lead, fast) - nt(refl_r, side, fast)


def solution(mesh):
    shape = (mesh.shape["row"] // 2, 2, 4, mesh.shape["col"] // 4)
    torus = Mesh(mesh.devices.reshape(shape), EVERY)
    return jax.shard_map(
        per_device, mesh=torus, in_specs=(P(ROW, COL),), out_specs=P(ROW, COL), check_vma=False
    )
```

```python
import jax
import jax.numpy as jnp
from jax import lax
from jax.experimental import pallas as pl
from jax.experimental.pallas import tpu as pltpu
from jax.sharding import Mesh
from jax.sharding import PartitionSpec as P

ROW = ("y", "core")
COL = ("x", "z")
EVERY = ROW + COL
SIGN = 1.0


def dot(left, right, dims, precision):
    return lax.dot_general(
        left,
        right,
        (dims, ((), ())),
        precision=precision,
        preferred_element_type=jnp.float32,
    )


def mm(left, right, precision=lax.Precision.HIGHEST):
    return dot(left, right, ((1,), (0,)), precision)


def tn(left, right, precision=lax.Precision.HIGHEST):
    return dot(left, right, ((0,), (0,)), precision)


def nt(left, right, precision=lax.Precision.HIGHEST):
    return dot(left, right, ((1,), (1,)), precision)


def exchange(tiles, axis):
    return lax.all_to_all(tiles, axis, 0, 0, tiled=True)


def to_all(piece, axis):
    n = lax.axis_size(axis)
    return exchange(jnp.broadcast_to(piece[None], (n, *piece.shape)), axis)


def invert_half(m_ref, c_ref):
    n = m_ref.shape[0]
    lanes = lax.broadcasted_iota(jnp.int32, (n, n), 1)
    subs = lax.broadcasted_iota(jnp.int32, (n, n), 0)
    lane_row = lax.broadcasted_iota(jnp.int32, (1, n), 1)

    def step(k, carry):
        m = m_ref[...]
        hit = lanes == k
        col = jnp.sum(jnp.where(hit, m, 0.0), axis=1, keepdims=True)
        c_ref[...] = jnp.broadcast_to(col, (n, n))
        pivot = c_ref[pl.ds(k, 1), :]
        row = jnp.where(lane_row == k, 1.0, m_ref[pl.ds(k, 1), :]) / pivot
        rest = jnp.where(hit, 0.0, m) - c_ref[...] * row
        m_ref[...] = jnp.where(subs == k, row, rest)
        return carry

    lax.fori_loop(0, n, step, 0)


def first_half(a_ref, t11_ref, right_ref, left_ref, schur_ref, m_ref, c_ref):
    h = a_ref.shape[0] // 2
    m_ref[...] = a_ref[:h, :h]
    invert_half(m_ref, c_ref)
    t11 = m_ref[...]
    right = mm(t11, a_ref[:h, h:])
    t11_ref[...] = t11
    right_ref[...] = right
    left_ref[...] = mm(a_ref[h:, :h], t11)
    schur_ref[...] = a_ref[h:, h:] - mm(a_ref[h:, :h], right)


def second_half(t11_ref, right_ref, left_ref, schur_ref, out_ref, m_ref, c_ref):
    h = t11_ref.shape[0]
    m_ref[...] = schur_ref[...]
    invert_half(m_ref, c_ref)
    t22 = m_ref[...]
    up = mm(right_ref[...], t22)
    out_ref[:h, :h] = t11_ref[...] + mm(up, left_ref[...])
    out_ref[:h, h:] = -up
    out_ref[h:, :h] = -mm(t22, left_ref[...])
    out_ref[h:, h:] = t22


COST = pl.CostEstimate(flops=2_000_000_000, bytes_accessed=500_000, transcendentals=0)


def half_inverted(a):
    half = jax.ShapeDtypeStruct((a.shape[0] // 2, a.shape[1] // 2), jnp.float32)
    return pl.pallas_call(
        first_half,
        out_shape=[half] * 4,
        scratch_shapes=[pltpu.VMEM(half.shape, jnp.float32)] * 2,
        cost_estimate=COST,
    )(a)


def inverted(parts):
    h = parts[0].shape[0]
    return pl.pallas_call(
        second_half,
        out_shape=jax.ShapeDtypeStruct((2 * h, 2 * h), jnp.float32),
        scratch_shapes=[pltpu.VMEM((h, h), jnp.float32)] * 2,
        cost_estimate=COST,
    )(*parts)


def per_device(matrix):
    row_count, width = matrix.shape
    rows, xs, zs = lax.axis_size(ROW), lax.axis_size("x"), lax.axis_size("z")
    part = width // rows
    ratio = row_count // width
    row_id = lax.axis_index(ROW)
    col_id = lax.axis_index(COL)
    cols = xs * zs

    def to_block_row(piece):
        pairs = []
        for r in range(rows):
            for c in range(cols):
                pairs.append((r * cols + c, (c // ratio) * cols + (c % ratio) * rows + r))
        return lax.ppermute(piece, EVERY, pairs)

    first = (row_id == 0).astype(jnp.float32)
    fast = lax.Precision.HIGH

    panel_c0 = jnp.where(col_id > 0, matrix[:width].T, 0.0)
    head, below = matrix[:width], matrix[width:]
    gram_r = tn(below, below) + tn(head * (1.0 - first), head)
    both = exchange(
        jnp.concatenate(
            [panel_c0.reshape(rows, part, width), gram_r.reshape(rows, part, width)], axis=1
        ),
        ROW,
    )
    piece = both[0, :part]
    gram_piece = jnp.sum(both[:, part:], axis=0)
    with jax.named_scope("move_panel"):
        moved = to_block_row(piece)

    with jax.named_scope("lead_x"):
        lead = to_all(jnp.where(col_id == 0, gram_piece, piece), "x")[0]
    lead = to_all(lead, "z")[:2].reshape(2 * part, width)
    lead = to_all(lead, ROW)
    lead, moved = lax.optimization_barrier((lead, moved))
    gram = lead[:, :part].reshape(width, width)
    top = lead[:, part:].reshape(width, width)

    along_z = to_all(moved, "z").reshape(zs * part, width)
    panel_r = to_all(along_z, "x").reshape(row_count, width)
    low = lax.linalg.cholesky(gram, symmetrize_input=False)
    upper = SIGN * low.T
    parts = half_inverted(gram + SIGN * mm(low, top))
    is_lead = jnp.logical_and(row_id == 0, lax.axis_index("x") == 1)
    refl_z = along_z + jnp.where(is_lead, upper, 0.0)
    refl_r = lax.dynamic_update_slice_in_dim(
        panel_r, panel_r[width : 2 * width] + first * upper, width, 0
    )

    x_part = tn(matrix, refl_r, fast)
    x_piece = jnp.sum(exchange(x_part.reshape(rows, part, width), ROW), axis=0)
    x_z = to_all(to_block_row(x_piece), "z").reshape(zs * part, width)

    y_part = tn(refl_z, x_z, fast)
    own = jnp.concatenate([x_piece, piece], axis=0)
    own = jnp.broadcast_to(own[None], (rows, 2 * part, width))
    both = jnp.concatenate([own, y_part.reshape(rows, part, width)], axis=1)
    both, parts = lax.optimization_barrier((both, parts))
    both = exchange(both, ROW)
    tfac = inverted(parts)
    x_c = both[:, :part].reshape(width, width)
    panel_c = both[:, part : 2 * part].reshape(width, width)
    refl_c = panel_c + jnp.where(col_id == 1, upper, 0.0)
    y_piece = jnp.sum(both[:, 2 * part :], axis=0)

    both, tfac = lax.optimization_barrier((jnp.concatenate([x_z, y_piece], axis=0), tfac))
    both = to_all(both, "x")
    x_r = both[:, : zs * part].reshape(row_count, width)
    y_piece = jnp.sum(both[:, zs * part :], axis=0)
    y_full = to_all(y_piece, ROW).reshape(width, width)

    middle = tn(tfac, mm(y_full, tfac))
    side = mm(x_c, tfac) - mm(refl_c, middle)
    lead = nt(refl_c, tfac)
    return matrix - nt(x_r, lead, fast) - nt(refl_r, side, fast)


def solution(mesh):
    shape = (mesh.shape["row"] // 2, 2, 4, mesh.shape["col"] // 4)
    torus = Mesh(mesh.devices.reshape(shape), EVERY)
    return jax.shard_map(
        per_device, mesh=torus, in_specs=(P(ROW, COL),), out_specs=P(ROW, COL), check_vma=False
    )
```

```python
import jax
import jax.numpy as jnp
from jax import lax
from jax.experimental import pallas as pl
from jax.experimental.pallas import tpu as pltpu
from jax.sharding import Mesh
from jax.sharding import PartitionSpec as P

ROW = ("y", "core")
COL = ("x", "z")
EVERY = ROW + COL
SIGN = 1.0


def dot(left, right, dims, precision):
    return lax.dot_general(
        left,
        right,
        (dims, ((), ())),
        precision=precision,
        preferred_element_type=jnp.float32,
    )


def mm(left, right, precision=lax.Precision.HIGHEST):
    return dot(left, right, ((1,), (0,)), precision)


def tn(left, right, precision=lax.Precision.HIGHEST):
    return dot(left, right, ((0,), (0,)), precision)


def nt(left, right, precision=lax.Precision.HIGHEST):
    return dot(left, right, ((1,), (1,)), precision)


def exchange(tiles, axis):
    return lax.all_to_all(tiles, axis, 0, 0, tiled=True)


def to_all(piece, axis):
    n = lax.axis_size(axis)
    return exchange(jnp.broadcast_to(piece[None], (n, *piece.shape)), axis)


def invert_half(m_ref, c_ref):
    n = m_ref.shape[0]
    lanes = lax.broadcasted_iota(jnp.int32, (n, n), 1)
    subs = lax.broadcasted_iota(jnp.int32, (n, n), 0)
    lane_row = lax.broadcasted_iota(jnp.int32, (1, n), 1)

    def step(k, carry):
        m = m_ref[...]
        hit = lanes == k
        col = jnp.sum(jnp.where(hit, m, 0.0), axis=1, keepdims=True)
        c_ref[...] = jnp.broadcast_to(col, (n, n))
        pivot = c_ref[pl.ds(k, 1), :]
        row = jnp.where(lane_row == k, 1.0, m_ref[pl.ds(k, 1), :]) / pivot
        rest = jnp.where(hit, 0.0, m) - c_ref[...] * row
        m_ref[...] = jnp.where(subs == k, row, rest)
        return carry

    lax.fori_loop(0, n, step, 0)


def first_half(a_ref, t11_ref, right_ref, left_ref, schur_ref, m_ref, c_ref):
    h = a_ref.shape[0] // 2
    m_ref[...] = a_ref[:h, :h]
    invert_half(m_ref, c_ref)
    t11 = m_ref[...]
    right = mm(t11, a_ref[:h, h:])
    t11_ref[...] = t11
    right_ref[...] = right
    left_ref[...] = mm(a_ref[h:, :h], t11)
    schur_ref[...] = a_ref[h:, h:] - mm(a_ref[h:, :h], right)


def second_half(t11_ref, right_ref, left_ref, schur_ref, out_ref, m_ref, c_ref):
    h = t11_ref.shape[0]
    m_ref[...] = schur_ref[...]
    invert_half(m_ref, c_ref)
    t22 = m_ref[...]
    up = mm(right_ref[...], t22)
    out_ref[:h, :h] = t11_ref[...] + mm(up, left_ref[...])
    out_ref[:h, h:] = -up
    out_ref[h:, :h] = -mm(t22, left_ref[...])
    out_ref[h:, h:] = t22


COST = pl.CostEstimate(flops=2_000_000_000, bytes_accessed=500_000, transcendentals=0)


def half_inverted(a):
    half = jax.ShapeDtypeStruct((a.shape[0] // 2, a.shape[1] // 2), jnp.float32)
    return pl.pallas_call(
        first_half,
        out_shape=[half] * 4,
        scratch_shapes=[pltpu.VMEM(half.shape, jnp.float32)] * 2,
        cost_estimate=COST,
    )(a)


def inverted(parts):
    h = parts[0].shape[0]
    return pl.pallas_call(
        second_half,
        out_shape=jax.ShapeDtypeStruct((2 * h, 2 * h), jnp.float32),
        scratch_shapes=[pltpu.VMEM((h, h), jnp.float32)] * 2,
        cost_estimate=COST,
    )(*parts)


GROUP = 4


def eliminate(m_ref, c_ref, u_ref):
    n, w = m_ref.shape
    lanes = lax.broadcasted_iota(jnp.int32, (n, n), 1)
    subs = lax.broadcasted_iota(jnp.int32, (n, n), 0)

    def wide(x):
        return jnp.concatenate([x] * (w // n), axis=1)

    def step(trip, carry):
        k = trip * GROUP
        square = m_ref[:, :n]
        cols, rows = [], []
        for j in range(GROUP):
            col = jnp.sum(jnp.where(lanes == k + j, square, 0.0), axis=1, keepdims=True)
            col = jnp.broadcast_to(col, (n, n))
            cols.append(col)
            c_ref[j] = col
            rows.append(m_ref[pl.ds(k + j, 1), :])
        for j in range(GROUP):
            pivot = c_ref[j, pl.ds(k + j, 1), :]
            scale = lax.rsqrt(pivot)
            scale = scale * (1.5 - 0.5 * pivot * scale * scale)
            cols[j] = cols[j] * scale
            rows[j] = rows[j] * wide(scale)
            u_ref[j] = cols[j]
            for i in range(j + 1, GROUP):
                factor = u_ref[j, pl.ds(k + i, 1), :]
                cols[i] = cols[i] - cols[j] * factor
                rows[i] = rows[i] - rows[j] * wide(factor)
                if i == j + 1:
                    c_ref[i] = cols[i]
        rest = m_ref[...]
        below = subs >= k + GROUP
        for j in range(GROUP):
            rest = rest - wide(jnp.where(below, cols[j], 0.0)) * rows[j]
        m_ref[...] = rest
        for j in range(GROUP):
            m_ref[pl.ds(k + j, 1), :] = rows[j]
        return carry

    lax.fori_loop(0, n // GROUP, step, 0)


def upper_part(x):
    subs = lax.broadcasted_iota(jnp.int32, x.shape, 0)
    lanes = lax.broadcasted_iota(jnp.int32, x.shape, 1)
    return jnp.where(subs <= lanes, x, 0.0)


def first_rows(g_ref, rows_ref, schur_ref, m_ref, c_ref, u_ref):
    h = m_ref.shape[0]
    m_ref[...] = g_ref[:h, :]
    eliminate(m_ref, c_ref, u_ref)
    right = m_ref[:, h:]
    rows_ref[:, :h] = upper_part(m_ref[:, :h])
    rows_ref[:, h:] = right
    schur_ref[...] = g_ref[h:, h:] - tn(right, right)


def last_rows(rows_ref, schur_ref, out_ref, m_ref, c_ref, u_ref):
    h = m_ref.shape[0]
    m_ref[...] = schur_ref[...]
    eliminate(m_ref, c_ref, u_ref)
    out_ref[:h, :] = rows_ref[...]
    out_ref[h:, :h] = jnp.zeros((h, h), jnp.float32)
    out_ref[h:, h:] = upper_part(m_ref[...])


def half_factored(gram):
    n = gram.shape[0]
    h = n // 2
    return pl.pallas_call(
        first_rows,
        out_shape=[
            jax.ShapeDtypeStruct((h, n), jnp.float32),
            jax.ShapeDtypeStruct((h, h), jnp.float32),
        ],
        scratch_shapes=[pltpu.VMEM((h, n), jnp.float32)]
        + [pltpu.VMEM((GROUP, h, h), jnp.float32)] * 2,
        cost_estimate=COST,
    )(gram)


def factored(rows, schur):
    h, n = rows.shape
    return pl.pallas_call(
        last_rows,
        out_shape=jax.ShapeDtypeStruct((n, n), jnp.float32),
        scratch_shapes=[pltpu.VMEM((h, h), jnp.float32)]
        + [pltpu.VMEM((GROUP, h, h), jnp.float32)] * 2,
        cost_estimate=COST,
    )(rows, schur)


def per_device(matrix):
    row_count, width = matrix.shape
    rows, xs, zs = lax.axis_size(ROW), lax.axis_size("x"), lax.axis_size("z")
    part = width // rows
    ratio = row_count // width
    row_id = lax.axis_index(ROW)
    col_id = lax.axis_index(COL)
    cols = xs * zs

    def to_block_row(piece):
        pairs = []
        for r in range(rows):
            for c in range(cols):
                pairs.append((r * cols + c, (c // ratio) * cols + (c % ratio) * rows + r))
        return lax.ppermute(piece, EVERY, pairs)

    first = (row_id == 0).astype(jnp.float32)
    fast = lax.Precision.HIGH

    panel_c0 = jnp.where(col_id > 0, matrix[:width].T, 0.0)
    head, below = matrix[:width], matrix[width:]
    gram_r = tn(below, below) + tn(head * (1.0 - first), head)
    both = exchange(
        jnp.concatenate(
            [panel_c0.reshape(rows, part, width), gram_r.reshape(rows, part, width)], axis=1
        ),
        ROW,
    )
    piece = both[0, :part]
    gram_piece = jnp.sum(both[:, part:], axis=0)
    with jax.named_scope("move_panel"):
        moved = to_block_row(piece)

    with jax.named_scope("lead_x"):
        lead = to_all(jnp.where(col_id == 0, gram_piece, piece), "x")[0]
    lead = to_all(lead, "z")[:2].reshape(2 * part, width)
    lead = to_all(lead, ROW)
    lead, moved = lax.optimization_barrier((lead, moved))
    gram = lead[:, :part].reshape(width, width)
    top = lead[:, part:].reshape(width, width)

    along_z = to_all(moved, "z").reshape(zs * part, width)
    halves = half_factored(gram)
    along_z, halves = lax.optimization_barrier((along_z, halves))
    panel_r = to_all(along_z, "x").reshape(row_count, width)
    factor = factored(*halves)
    panel_r, factor = lax.optimization_barrier((panel_r, factor))
    upper = SIGN * factor
    parts = half_inverted(gram + tn(upper, top))
    is_lead = jnp.logical_and(row_id == 0, lax.axis_index("x") == 1)
    refl_z = along_z + jnp.where(is_lead, upper, 0.0)
    refl_r = lax.dynamic_update_slice_in_dim(
        panel_r, panel_r[width : 2 * width] + first * upper, width, 0
    )

    x_part = tn(matrix, refl_r, fast)
    x_piece = jnp.sum(exchange(x_part.reshape(rows, part, width), ROW), axis=0)
    x_z = to_all(to_block_row(x_piece), "z").reshape(zs * part, width)

    y_part = tn(refl_z, x_z, fast)
    own = jnp.concatenate([x_piece, piece], axis=0)
    own = jnp.broadcast_to(own[None], (rows, 2 * part, width))
    both = jnp.concatenate([own, y_part.reshape(rows, part, width)], axis=1)
    both, parts = lax.optimization_barrier((both, parts))
    both = exchange(both, ROW)
    tfac = inverted(parts)
    x_c = both[:, :part].reshape(width, width)
    panel_c = both[:, part : 2 * part].reshape(width, width)
    refl_c = panel_c + jnp.where(col_id == 1, upper, 0.0)
    y_piece = jnp.sum(both[:, 2 * part :], axis=0)

    both, tfac = lax.optimization_barrier((jnp.concatenate([x_z, y_piece], axis=0), tfac))
    both = to_all(both, "x")
    x_r = both[:, : zs * part].reshape(row_count, width)
    y_piece = jnp.sum(both[:, zs * part :], axis=0)
    y_full = to_all(y_piece, ROW).reshape(width, width)

    middle = tn(tfac, mm(y_full, tfac))
    side = mm(x_c, tfac) - mm(refl_c, middle)
    lead = nt(refl_c, tfac)
    return matrix - nt(x_r, lead, fast) - nt(refl_r, side, fast)


def solution(mesh):
    shape = (mesh.shape["row"] // 2, 2, 4, mesh.shape["col"] // 4)
    torus = Mesh(mesh.devices.reshape(shape), EVERY)
    return jax.shard_map(
        per_device, mesh=torus, in_specs=(P(ROW, COL),), out_specs=P(ROW, COL), check_vma=False
    )
```

```python
import jax
import jax.numpy as jnp
from jax import lax
from jax.experimental import pallas as pl
from jax.experimental.pallas import tpu as pltpu
from jax.sharding import Mesh
from jax.sharding import PartitionSpec as P

ROW = ("y", "core")
COL = ("x", "z")
EVERY = ROW + COL
SIGN = 1.0


def dot(left, right, dims, precision):
    return lax.dot_general(
        left,
        right,
        (dims, ((), ())),
        precision=precision,
        preferred_element_type=jnp.float32,
    )


def mm(left, right, precision=lax.Precision.HIGHEST):
    return dot(left, right, ((1,), (0,)), precision)


def tn(left, right, precision=lax.Precision.HIGHEST):
    return dot(left, right, ((0,), (0,)), precision)


def nt(left, right, precision=lax.Precision.HIGHEST):
    return dot(left, right, ((1,), (1,)), precision)


def exchange(tiles, axis):
    return lax.all_to_all(tiles, axis, 0, 0, tiled=True)


def to_all(piece, axis):
    n = lax.axis_size(axis)
    return exchange(jnp.broadcast_to(piece[None], (n, *piece.shape)), axis)


GROUP = 4


def invert_half(m_ref, c_ref):
    n = m_ref.shape[0]
    lanes = lax.broadcasted_iota(jnp.int32, (n, n), 1)
    subs = lax.broadcasted_iota(jnp.int32, (n, n), 0)
    lane_row = lax.broadcasted_iota(jnp.int32, (1, n), 1)

    def step(trip, carry):
        k = trip * GROUP
        m = m_ref[...]
        cols, rows, used = [], [], []
        for j in range(GROUP):
            col = jnp.sum(jnp.where(lanes == k + j, m, 0.0), axis=1, keepdims=True)
            cols.append(jnp.broadcast_to(col, (n, n)))
            c_ref[j] = cols[j]
            rows.append(m_ref[pl.ds(k + j, 1), :])
        for j in range(GROUP):
            pivot = c_ref[j, pl.ds(k + j, 1), :]
            row = jnp.where(lane_row == k + j, 1.0, rows[j]) / pivot
            for i in range(GROUP):
                if i != j:
                    factor = c_ref[j, pl.ds(k + i, 1), :]
                    rows[i] = jnp.where(lane_row == k + j, 0.0, rows[i]) - factor * row
            rows[j] = row
            for i in range(j + 1, GROUP):
                entry = c_ref[i, pl.ds(k + j, 1), :] / pivot
                cols[i] = jnp.where(subs == k + j, entry, cols[i] - cols[j] * entry)
                c_ref[i] = cols[i]
            later = jnp.logical_and(lane_row > k + j, lane_row < k + GROUP)
            used.append(jnp.where(later, 0.0, row))
        rest = jnp.where(jnp.logical_and(lanes >= k, lanes < k + GROUP), 0.0, m)
        for j in range(GROUP):
            rest = rest - cols[j] * used[j]
        m_ref[...] = rest
        for j in range(GROUP):
            m_ref[pl.ds(k + j, 1), :] = rows[j]
        return carry

    lax.fori_loop(0, n // GROUP, step, 0)


def first_half(a_ref, t11_ref, right_ref, left_ref, schur_ref, m_ref, c_ref):
    h = a_ref.shape[0] // 2
    m_ref[...] = a_ref[:h, :h]
    invert_half(m_ref, c_ref)
    t11 = m_ref[...]
    right = mm(t11, a_ref[:h, h:])
    t11_ref[...] = t11
    right_ref[...] = right
    left_ref[...] = mm(a_ref[h:, :h], t11)
    schur_ref[...] = a_ref[h:, h:] - mm(a_ref[h:, :h], right)


def second_half(t11_ref, right_ref, left_ref, schur_ref, out_ref, m_ref, c_ref):
    h = t11_ref.shape[0]
    m_ref[...] = schur_ref[...]
    invert_half(m_ref, c_ref)
    t22 = m_ref[...]
    up = mm(right_ref[...], t22)
    out_ref[:h, :h] = t11_ref[...] + mm(up, left_ref[...])
    out_ref[:h, h:] = -up
    out_ref[h:, :h] = -mm(t22, left_ref[...])
    out_ref[h:, h:] = t22


COST = pl.CostEstimate(flops=2_000_000_000, bytes_accessed=500_000, transcendentals=0)


def half_inverted(a):
    half = jax.ShapeDtypeStruct((a.shape[0] // 2, a.shape[1] // 2), jnp.float32)
    return pl.pallas_call(
        first_half,
        out_shape=[half] * 4,
        scratch_shapes=[
            pltpu.VMEM(half.shape, jnp.float32),
            pltpu.VMEM((GROUP, *half.shape), jnp.float32),
        ],
        cost_estimate=COST,
    )(a)


def inverted(parts):
    h = parts[0].shape[0]
    return pl.pallas_call(
        second_half,
        out_shape=jax.ShapeDtypeStruct((2 * h, 2 * h), jnp.float32),
        scratch_shapes=[
            pltpu.VMEM((h, h), jnp.float32),
            pltpu.VMEM((GROUP, h, h), jnp.float32),
        ],
        cost_estimate=COST,
    )(*parts)


def eliminate(m_ref, c_ref, u_ref):
    n, w = m_ref.shape
    lanes = lax.broadcasted_iota(jnp.int32, (n, n), 1)
    subs = lax.broadcasted_iota(jnp.int32, (n, n), 0)

    def wide(x):
        return jnp.concatenate([x] * (w // n), axis=1)

    def step(trip, carry):
        k = trip * GROUP
        square = m_ref[:, :n]
        cols, rows = [], []
        for j in range(GROUP):
            col = jnp.sum(jnp.where(lanes == k + j, square, 0.0), axis=1, keepdims=True)
            col = jnp.broadcast_to(col, (n, n))
            cols.append(col)
            c_ref[j] = col
            rows.append(m_ref[pl.ds(k + j, 1), :])
        for j in range(GROUP):
            pivot = c_ref[j, pl.ds(k + j, 1), :]
            scale = lax.rsqrt(pivot)
            scale = scale * (1.5 - 0.5 * pivot * scale * scale)
            cols[j] = cols[j] * scale
            rows[j] = rows[j] * wide(scale)
            u_ref[j] = cols[j]
            for i in range(j + 1, GROUP):
                factor = u_ref[j, pl.ds(k + i, 1), :]
                cols[i] = cols[i] - cols[j] * factor
                rows[i] = rows[i] - rows[j] * wide(factor)
                if i == j + 1:
                    c_ref[i] = cols[i]
        rest = m_ref[...]
        below = subs >= k + GROUP
        for j in range(GROUP):
            rest = rest - wide(jnp.where(below, cols[j], 0.0)) * rows[j]
        m_ref[...] = rest
        for j in range(GROUP):
            m_ref[pl.ds(k + j, 1), :] = rows[j]
        return carry

    lax.fori_loop(0, n // GROUP, step, 0)


def upper_part(x):
    subs = lax.broadcasted_iota(jnp.int32, x.shape, 0)
    lanes = lax.broadcasted_iota(jnp.int32, x.shape, 1)
    return jnp.where(subs <= lanes, x, 0.0)


def first_rows(g_ref, rows_ref, schur_ref, m_ref, c_ref, u_ref):
    h = m_ref.shape[0]
    m_ref[...] = g_ref[:h, :]
    eliminate(m_ref, c_ref, u_ref)
    right = m_ref[:, h:]
    rows_ref[:, :h] = upper_part(m_ref[:, :h])
    rows_ref[:, h:] = right
    schur_ref[...] = g_ref[h:, h:] - tn(right, right)


def last_rows(rows_ref, schur_ref, out_ref, m_ref, c_ref, u_ref):
    h = m_ref.shape[0]
    m_ref[...] = schur_ref[...]
    eliminate(m_ref, c_ref, u_ref)
    out_ref[:h, :] = rows_ref[...]
    out_ref[h:, :h] = jnp.zeros((h, h), jnp.float32)
    out_ref[h:, h:] = upper_part(m_ref[...])


def half_factored(gram):
    n = gram.shape[0]
    h = n // 2
    return pl.pallas_call(
        first_rows,
        out_shape=[
            jax.ShapeDtypeStruct((h, n), jnp.float32),
            jax.ShapeDtypeStruct((h, h), jnp.float32),
        ],
        scratch_shapes=[pltpu.VMEM((h, n), jnp.float32)]
        + [pltpu.VMEM((GROUP, h, h), jnp.float32)] * 2,
        cost_estimate=COST,
    )(gram)


def factored(rows, schur):
    h, n = rows.shape
    return pl.pallas_call(
        last_rows,
        out_shape=jax.ShapeDtypeStruct((n, n), jnp.float32),
        scratch_shapes=[pltpu.VMEM((h, h), jnp.float32)]
        + [pltpu.VMEM((GROUP, h, h), jnp.float32)] * 2,
        cost_estimate=COST,
    )(rows, schur)


def per_device(matrix):
    row_count, width = matrix.shape
    rows, xs, zs = lax.axis_size(ROW), lax.axis_size("x"), lax.axis_size("z")
    part = width // rows
    ratio = row_count // width
    row_id = lax.axis_index(ROW)
    col_id = lax.axis_index(COL)
    cols = xs * zs

    def to_block_row(piece):
        pairs = []
        for r in range(rows):
            for c in range(cols):
                pairs.append((r * cols + c, (c // ratio) * cols + (c % ratio) * rows + r))
        return lax.ppermute(piece, EVERY, pairs)

    first = (row_id == 0).astype(jnp.float32)
    fast = lax.Precision.HIGH

    panel_c0 = jnp.where(col_id > 0, matrix[:width].T, 0.0)
    head, below = matrix[:width], matrix[width:]
    gram_r = tn(below, below) + tn(head * (1.0 - first), head)
    both = exchange(
        jnp.concatenate(
            [panel_c0.reshape(rows, part, width), gram_r.reshape(rows, part, width)], axis=1
        ),
        ROW,
    )
    piece = both[0, :part]
    gram_piece = jnp.sum(both[:, part:], axis=0)
    with jax.named_scope("move_panel"):
        moved = to_block_row(piece)

    with jax.named_scope("lead_x"):
        lead = to_all(jnp.where(col_id == 0, gram_piece, piece), "x")[0]
    lead = to_all(lead, "z")[:2].reshape(2 * part, width)
    lead = to_all(lead, ROW)
    lead, moved = lax.optimization_barrier((lead, moved))
    gram = lead[:, :part].reshape(width, width)
    top = lead[:, part:].reshape(width, width)

    along_z = to_all(moved, "z").reshape(zs * part, width)
    halves = half_factored(gram)
    along_z, halves = lax.optimization_barrier((along_z, halves))
    panel_r = to_all(along_z, "x").reshape(row_count, width)
    factor = factored(*halves)
    panel_r, factor = lax.optimization_barrier((panel_r, factor))
    upper = SIGN * factor
    parts = half_inverted(gram + tn(upper, top))
    is_lead = jnp.logical_and(row_id == 0, lax.axis_index("x") == 1)
    refl_z = along_z + jnp.where(is_lead, upper, 0.0)
    refl_r = lax.dynamic_update_slice_in_dim(
        panel_r, panel_r[width : 2 * width] + first * upper, width, 0
    )

    x_part = tn(matrix, refl_r, fast)
    x_piece = jnp.sum(exchange(x_part.reshape(rows, part, width), ROW), axis=0)
    x_moved, parts = lax.optimization_barrier((to_block_row(x_piece), parts))
    x_z = to_all(x_moved, "z").reshape(zs * part, width)
    x_z, parts = lax.optimization_barrier((x_z, parts))

    y_part = tn(refl_z, x_z, fast)
    own = jnp.concatenate([x_piece, piece], axis=0)
    own = jnp.broadcast_to(own[None], (rows, 2 * part, width))
    both = jnp.concatenate([own, y_part.reshape(rows, part, width)], axis=1)
    both = exchange(both, ROW)
    tfac = inverted(parts)
    x_c = both[:, :part].reshape(width, width)
    panel_c = both[:, part : 2 * part].reshape(width, width)
    refl_c = panel_c + jnp.where(col_id == 1, upper, 0.0)
    y_piece = jnp.sum(both[:, 2 * part :], axis=0)

    both, tfac = lax.optimization_barrier((jnp.concatenate([x_z, y_piece], axis=0), tfac))
    both = to_all(both, "x")
    x_r = both[:, : zs * part].reshape(row_count, width)
    y_piece = jnp.sum(both[:, zs * part :], axis=0)
    y_full = to_all(y_piece, ROW).reshape(width, width)

    middle = tn(tfac, mm(y_full, tfac))
    side = mm(x_c, tfac) - mm(refl_c, middle)
    lead = nt(refl_c, tfac)
    return matrix - nt(x_r, lead, fast) - nt(refl_r, side, fast)


def solution(mesh):
    shape = (mesh.shape["row"] // 2, 2, 4, mesh.shape["col"] // 4)
    torus = Mesh(mesh.devices.reshape(shape), EVERY)
    return jax.shard_map(
        per_device, mesh=torus, in_specs=(P(ROW, COL),), out_specs=P(ROW, COL), check_vma=False
    )
```
